32 devices in a mesh: node: 4 (over y, x), torus: 8 (over z, core).
Axes of the slice: x: 2, y: 2, z: 4, core: 2. Of those that a mesh axis runs over, the one named last changes fastest.
Arguments:
- tokens: bfloat16 [4096, 7168], P(('node', 'torus')), may hold values from -6 to 6
- expert_ids: int32 [4096, 8], P(('node', 'torus')), may hold values from 0 to 383, as said below
- route_weight: bfloat16 [4096, 8], P(('node', 'torus')), may hold values from 0.19921875 to 2.5
- w_gate: bfloat16 [16, 7168, 1024], P('torus', None, 'node'), may hold values from -0.0625 to 0.0625
- w_up: bfloat16 [16, 7168, 1024], P('torus', None, 'node'), may hold values from -0.0625 to 0.0625
- w_down: bfloat16 [16, 1024, 7168], P('torus', 'node'), may hold values from -0.1875 to 0.1875
Outputs:
- moe_out: bfloat16 [4096, 7168], P(('node', 'torus'))
The draws below stay inside these ranges and needn't reach their ends.
Inputs may be any that keep to these rules, and one draw needn't show every extreme that they name: `expert_ids`: each row names 8 different experts. Counting an expert e below 16 as one of group e // 2, at most 4 of the 128 rows of one device (aligned blocks of rows, in order) name an expert of any one group, and in every draw some group is named by exactly 4 rows of every device.
All inputs are finite; a program needn't handle non-finite values.
Results may differ from the reference program's by a relative error of at most 0.0095.
Values may be sent and summed in bfloat16 or wider, within the bound.
A program may use at most 128 MiB of HBM per device.

```python
import math
import jax
import jax.numpy as jnp
from jax import lax

D = 7168
FF = 1024
EXPERTS = 384
TOPK = 8
EXP_DEV = 2
CAP = 4
QBLOCK = 128
TOK_DEV = 128
GROUPS = 8
SOURCES = 32
WIN_EXPERTS = 16
TOKENS = 4096
N_NODE = 4


def draw_expert_ids(key, part):
    keys = jax.random.split(jax.random.fold_in(key, 17), 8)
    group_ids = jnp.arange(GROUPS, dtype=jnp.int32)
    hot_group = jax.random.randint(keys[0], (), 0, GROUPS, dtype=jnp.int32)
    second_group = jax.random.randint(keys[1], (SOURCES,), 0, GROUPS, dtype=jnp.int32)
    second_used = jax.random.randint(keys[2], (SOURCES,), 0, 2, dtype=jnp.int32)
    counts = jax.random.randint(keys[3], (SOURCES, GROUPS), 1, 4, dtype=jnp.int32)
    counts = jnp.where(group_ids[None, :] == hot_group, CAP, counts)
    counts = jnp.where((group_ids[None, :] == second_group[:, None]) & (second_used[:, None] == 1), CAP, counts)
    ends = jnp.cumsum(counts, axis=1).astype(jnp.int32)
    laps = TOPK // EXP_DEV
    position = jnp.arange(laps * TOK_DEV, dtype=jnp.int32).reshape(laps, TOK_DEV)
    owner = jnp.sum((ends[:, None, None, :] <= position[None, :, :, None]).astype(jnp.int32), axis=-1)
    inside = position[None, :, :] < ends[:, -1][:, None, None]
    picked = jax.random.randint(keys[4], (SOURCES, laps, TOK_DEV), 0, 3, dtype=jnp.int32)
    first = EXP_DEV * owner + (picked == 1).astype(jnp.int32)
    second = EXP_DEV * owner + 1
    first = jnp.where(inside, first, -1)
    second = jnp.where(inside & (picked == 2), second, -1)
    paired = jnp.stack([first, second], axis=2)
    slots = paired.reshape(SOURCES, TOPK, TOK_DEV).transpose(0, 2, 1)
    shuffles = jax.vmap(lambda sub: jax.random.permutation(sub, TOK_DEV))(jax.random.split(keys[5], SOURCES))
    inverse = jnp.argsort(shuffles, axis=1).astype(jnp.int32)
    slots = jnp.take_along_axis(slots, inverse[:, :, None], axis=1)
    remain = EXPERTS - WIN_EXPERTS
    offset = jax.random.randint(keys[6], (SOURCES, TOK_DEV, 1), 0, remain, dtype=jnp.int32)
    filler = WIN_EXPERTS + (offset + jnp.arange(TOPK, dtype=jnp.int32)[None, None, :]) % remain
    chosen = jnp.where(slots >= 0, slots, filler)
    scores = jax.random.randint(keys[7], (SOURCES, TOK_DEV, TOPK), 0, 1 << 20, dtype=jnp.int32) * TOPK + jnp.arange(TOPK, dtype=jnp.int32)[None, None, :]
    order = jnp.argsort(scores, axis=-1, stable=True)
    chosen = jnp.take_along_axis(chosen, order, axis=-1)
    return chosen.reshape(TOKENS, TOPK).astype(jnp.int32)


def steps_of(stream_key, dims, cuts, least, high):
    gain, own = 1.0, jax.random.fold_in(stream_key, 6)
    for axis_at, shards_of in cuts:
        draws = jnp.exp(jax.random.uniform(jax.random.fold_in(own, axis_at), (shards_of,), jnp.float32, least / len(cuts), high / len(cuts)))
        gain = gain * jnp.repeat(draws, dims[axis_at] // shards_of).reshape([-1 if axis == axis_at else 1 for axis in range(len(dims))])
    return gain


def centred(stream_key, shape, width, bound, cuts=(), held_as=jnp.bfloat16):
    loudness = steps_of(stream_key, shape, cuts, -0.22, 0.18) if cuts else 1.0
    drawn = jax.random.normal(stream_key, shape, jnp.float32) * width * loudness
    return jnp.minimum(jnp.maximum(drawn, -bound), bound).astype(held_as)


def setup_inputs(seed: int = 0) -> dict:
    streams_of = jax.random.split(jax.random.key(seed), 7)
    tokens = centred(streams_of[0], (TOKENS, D), 1.0, 6.0, ((0, 32),))
    expert_ids = draw_expert_ids(jax.random.fold_in(streams_of[6], 71), 0)
    route_weight = jnp.clip(jnp.exp(math.log(2.5) - 2.5296425 * jax.random.uniform(streams_of[2], (TOKENS, TOPK), jnp.float32) ** steps_of(streams_of[2], (TOKENS, TOPK), ((0, 32),), -0.2, 0.2)), 0.19921875, 2.5).astype(jnp.bfloat16)
    w_gate = centred(streams_of[3], (WIN_EXPERTS, D, FF), D ** -0.5, 0.0625, ((0, 8), (2, 4)))
    w_up = centred(streams_of[4], (WIN_EXPERTS, D, FF), D ** -0.5, 0.0625, ((0, 8), (2, 4)))
    w_down = centred(streams_of[5], (WIN_EXPERTS, FF, D), FF ** -0.5, 0.1875, ((0, 8), (1, 4)))
    return {"tokens": tokens, "expert_ids": expert_ids, "route_weight": route_weight, "w_gate": w_gate, "w_up": w_up, "w_down": w_down}


block_rows = 64


def quantize(tokens):
    count = tokens.shape[0]
    blocks = tokens.astype(jnp.float32).reshape(count, -1, QBLOCK)
    largest = jnp.max(jnp.abs(blocks), axis=-1)
    scale = ((largest + 1e-6) * (1.0 / 448.0)).astype(jnp.bfloat16)
    scale = lax.optimization_barrier(scale)
    quantized = (blocks / scale.astype(jnp.float32)[:, :, None]).astype(jnp.bfloat16)
    quantized = lax.optimization_barrier(quantized)
    return quantized.reshape(count, -1), scale


def restore(quantized, scale):
    count = quantized.shape[0]
    blocks = quantized.astype(jnp.float32).reshape(count, -1, QBLOCK) * scale.astype(jnp.float32)[:, :, None]
    return blocks.astype(jnp.bfloat16).reshape(count, -1)


def reference(tokens, expert_ids, route_weight, w_gate, w_up, w_down):
    quantized, scale = quantize(tokens)
    restored = restore(quantized, scale)
    experts = jnp.arange(WIN_EXPERTS, dtype=jnp.int32)
    weight_float = route_weight.astype(jnp.float32)
    route_sel = jnp.zeros((TOKENS, WIN_EXPERTS), jnp.float32)
    named = jnp.zeros((TOKENS, WIN_EXPERTS), jnp.int32)
    for slot in range(TOPK):
        matched = expert_ids[:, slot:slot + 1] == experts[None, :]
        route_sel = route_sel + jnp.where(matched, weight_float[:, slot:slot + 1], jnp.float32(0.0))
        named = named + matched.astype(jnp.int32)
    member = named.reshape(TOKENS, GROUPS, EXP_DEV).sum(axis=-1)
    route_sel = route_sel.reshape(TOKENS, GROUPS, EXP_DEV)
    quarter = FF // N_NODE
    total = jnp.zeros((TOKENS, D), jnp.float32)
    offsets = jnp.arange(block_rows, dtype=jnp.int32)

    def group_step(group, total):
        inside = lax.dynamic_index_in_dim(member, group, 1, keepdims=False) > 0
        count = jnp.sum(inside.astype(jnp.int32)).astype(jnp.int32)
        order = jnp.argsort(jnp.where(inside, 0, 1).astype(jnp.int32), stable=True).astype(jnp.int32)
        order = jnp.concatenate([order, jnp.zeros((block_rows,), jnp.int32)])
        weights_group = lax.dynamic_index_in_dim(route_sel, group, 1, keepdims=False)
        gates = [lax.dynamic_index_in_dim(w_gate, EXP_DEV * group + expert, 0, keepdims=False) for expert in range(EXP_DEV)]
        ups = [lax.dynamic_index_in_dim(w_up, EXP_DEV * group + expert, 0, keepdims=False) for expert in range(EXP_DEV)]
        downs = [lax.dynamic_index_in_dim(w_down, EXP_DEV * group + expert, 0, keepdims=False) for expert in range(EXP_DEV)]

        def block_step(block, total):
            start = (block * block_rows).astype(jnp.int32)
            picked = lax.dynamic_slice_in_dim(order, start, block_rows)
            valid = (start + offsets) < count
            rows = restored[picked]
            weights = weights_group[picked]
            parts = [jnp.zeros((block_rows, D), jnp.float32) for piece in range(N_NODE)]
            for expert in range(EXP_DEV):
                gate = jnp.dot(rows, gates[expert], preferred_element_type=jnp.float32)
                upper = jnp.dot(rows, ups[expert], preferred_element_type=jnp.float32)
                hidden = (jax.nn.silu(gate) * upper).astype(jnp.bfloat16)
                for piece in range(N_NODE):
                    lower = piece * quarter
                    result = jnp.dot(hidden[:, lower:lower + quarter], downs[expert][lower:lower + quarter, :], preferred_element_type=jnp.float32)
                    parts[piece] = parts[piece] + weights[:, expert:expert + 1] * result
            combined = jnp.zeros((block_rows, D), jnp.float32)
            for piece in range(N_NODE):
                rounded = lax.optimization_barrier(parts[piece].astype(jnp.bfloat16))
                combined = combined + rounded.astype(jnp.float32)
            combined = lax.optimization_barrier(combined.astype(jnp.bfloat16))
            added = jnp.where(valid[:, None], combined.astype(jnp.float32), jnp.float32(0.0))
            return total.at[picked].add(added)

        blocks = (count + block_rows - 1) // block_rows
        return lax.fori_loop(0, blocks, block_step, total)

    total = lax.fori_loop(0, GROUPS, group_step, total)
    return total.astype(jnp.bfloat16)
```

```python
import functools

import jax
import jax.numpy as jnp
from jax import lax
from jax.experimental import pallas as pl
from jax.experimental.pallas import tpu as pltpu
from jax.sharding import PartitionSpec as P

CAP = 4
QBLOCK = 128
PARTS = 4
SUB = CAP * PARTS
CHUNK = 1024
WIDE = CHUNK // PARTS
MESH = pl.DeviceIdType.MESH
F32 = jnp.float32
BF16 = jnp.bfloat16

KINDS = (
    "z1", "z2", "z3", "x0", "x1", "x2", "x3", "y0", "y1", "y2", "y3",
    "fy0", "fy2", "fy3", "fx1", "fx2", "fx3",
    "ra0", "rb0", "gx0", "gy0", "zr0", "ra1", "rb1", "gx1", "gy1", "zr1",
    "wz", "wx", "wy", "wf",
)

TIMES = {
    "make": (0.0, 0.4),
    "late": (2.7, 0.01),
    "spread1": (1.75, 0.4),
    "forward0": (3.3, 0.45),
    "spread3": (4.4, 0.75),
    "forward1": (5.0, 0.5),
    "wspread": (6.0, 0.0),
    "forward3": (8.0, 1.0),
    "wforward": (9.0, 0.0),
    "spread2": (9.2, 0.6),
    "multiply1": (10.7, 1.0),
    "forward2": (12.2, 0.5),
    "warrived": (13.0, 0.0),
    "multiply0": (17.0, 0.45),
    "down1": (16.9, 0.35),
    "merge1": (19.4, 0.5),
    "home1": (22.0, 0.9),
    "down0": (20.5, 0.4),
    "merge0": (23.0, 0.6),
    "home0": (26.0, 0.95),
    "finish": (29.5, 0.95),
}


def flipped(index, mask):
    value = index
    bit = 0
    while mask >> bit:
        if (mask >> bit) & 1:
            size = 1 << bit
            value = value + size * (1 - 2 * lax.rem(lax.div(index, jnp.int32(size)), jnp.int32(2)))
        bit += 1
    return value


def dot(left, right):
    return jnp.dot(left, right, preferred_element_type=F32)


def kernel(
    groups, chunks,
    tok_hbm, ids_hbm, rw_hbm, wg_hbm, wu_hbm, wd_hbm, out_hbm,
    tok, ids, rw, wg, wu, wd, place, place_t, perm, perm_t,
    sent, held, wsent, warr, whold, xs, acc, hidden, wcol,
    part, relay_a, relay_b, got_x, got_y, back_s, back, obuf,
    ssems, rsems, lsems,
):
    node = lax.axis_index("node")
    torus = lax.axis_index("torus")
    rows = tok.shape[0]
    subs = groups * SUB
    fold = groups // 2
    sh = fold * SUB
    slots = fold * CAP
    lots = 4 * slots
    side = CHUNK // 2
    unit = min(128, sh)
    experts = wg.shape[0]
    peers = [j for j in range(groups) if not j & 2] + [j for j in range(groups) if j & 2]
    at_x = (flipped(node, 1), torus)
    at_y = (flipped(node, 2), torus)
    at_z = [(node, flipped(torus, j)) for j in range(groups)]

    barrier = pltpu.get_barrier_semaphore()
    for peer in at_z[1:] + [at_x, at_y]:
        pl.semaphore_signal(barrier, inc=1, device_id=peer, device_id_type=MESH)

    ids_cp = pltpu.make_async_copy(ids_hbm, ids, lsems.at[5, 0])
    rw_cp = pltpu.make_async_copy(rw_hbm, rw, lsems.at[5, 1])
    ids_cp.start()
    rw_cp.start()
    tok_cp, wg_cp, wu_cp, wd_cp = [], [], [], []
    for k in range(chunks):
        cols = pl.ds(k * CHUNK, CHUNK)
        tok_cp.append(pltpu.make_async_copy(tok_hbm.at[:, cols], tok.at[:, cols], lsems.at[0, k]))
        wg_cp.append(pltpu.make_async_copy(wg_hbm.at[:, cols, :], wg.at[:, cols, :], lsems.at[1, k]))
        wu_cp.append(pltpu.make_async_copy(wu_hbm.at[:, cols, :], wu.at[:, cols, :], lsems.at[2, k]))
        wd_cp.append(pltpu.make_async_copy(wd_hbm.at[:, :, cols], wd.at[:, :, cols], lsems.at[3, k]))
    for c in tok_cp:
        c.start()
    for a, b in zip(wg_cp, wu_cp):
        a.start()
        b.start()
    for c in wd_cp:
        c.start()

    pr = lax.broadcasted_iota(jnp.int32, (128, 128), 0)
    pc = lax.broadcasted_iota(jnp.int32, (128, 128), 1)
    ur = 128 // PARTS
    perm[...] = (pc == (pr % ur) * PARTS + pr // ur).astype(F32).astype(BF16)
    tr = lax.broadcasted_iota(jnp.int32, (unit, unit), 0)
    tc = lax.broadcasted_iota(jnp.int32, (unit, unit), 1)
    tu = unit // PARTS
    perm_t[...] = (tr == (tc % tu) * PARTS + tc // tu).astype(F32).astype(BF16)

    def distance(at):
        inner = at % fold
        return (inner // 2) * 4 + (at // fold) * 2 + inner % 2

    ids_cp.wait()
    rw_cp.wait()
    row = lax.broadcasted_iota(jnp.int32, (subs, rows), 0)
    gid = jnp.bitwise_xor(distance(row // SUB), jnp.full((subs, rows), torus, jnp.int32))
    slot_of = (row // PARTS) % CAP
    part_of = row % PARTS
    hit = jnp.zeros((subs, rows), F32)
    chosen = [jnp.zeros((subs, rows), F32) for _ in range(experts)]
    weights = rw[...].astype(F32)
    for k in range(ids.shape[0]):
        named = jnp.broadcast_to(ids[k : k + 1, :], (subs, rows))
        weight = jnp.broadcast_to(weights[k : k + 1, :], (subs, rows))
        for e in range(experts):
            same = named == gid * experts + e
            hit = jnp.where(same, 1.0, hit)
            chosen[e] = jnp.where(same, weight, chosen[e])
    lower = lax.broadcasted_iota(jnp.int32, (rows, rows), 0) < lax.broadcasted_iota(
        jnp.int32, (rows, rows), 1
    )
    before = dot(hit.astype(BF16), lower.astype(F32).astype(BF16))
    onehot = jnp.where(before == slot_of.astype(F32), hit, 0.0)
    for q in range(PARTS):
        place[q] = jnp.where(part_of == q, onehot, 0.0).astype(BF16)
    lane = lax.broadcasted_iota(jnp.int32, (subs, 128), 1)
    from_j = distance(lax.broadcasted_iota(jnp.int32, (subs, 128), 0) // SUB)
    wrow = jnp.zeros((subs, 128), F32)
    for e in range(experts):
        total = jnp.sum(onehot * chosen[e], axis=1, keepdims=True)
        wrow = jnp.where(lane == from_j * experts + e, total, wrow)
    wsent[...] = wrow.astype(BF16)
    warr[0:SUB] = wrow[0:SUB].astype(BF16)

    pl.semaphore_wait(barrier, groups + 1)

    def remote(kind, k, src, dst, peer):
        at = KINDS.index(kind)
        copy = pltpu.make_async_remote_copy(
            src_ref=src, dst_ref=dst, send_sem=ssems.at[at], recv_sem=rsems.at[at, k],
            device_id=peer, device_id_type=MESH,
        )
        copy.start()

    def wait(kind, k, ref):
        pltpu.make_async_copy(ref, ref, rsems.at[KINDS.index(kind), k]).wait()

    def sent_all(kind, ref):
        pltpu.make_async_copy(ref, ref, ssems.at[KINDS.index(kind)]).wait()

    def lanes(k):
        return pl.ds(k * WIDE, WIDE)

    classes = ((0, 0, 1), (0, 1, 2), (0, 2, fold), (1, 0, fold))

    def rows_of(c, r, k, lo=None, hi=None):
        h, first, last = classes[c]
        lo = first if lo is None else lo
        hi = last if hi is None else hi
        at = pl.ds(r * sh + lo * SUB, (hi - lo) * SUB)
        return held.at[h, at, :] if k is None else held.at[h, at, lanes(k)]

    def halves(c):
        h, lo, hi = classes[c]
        mid = {0: hi, 1: lo}.get(c, (lo + hi) // 2)
        return lo, mid, hi

    def exchange(c, k):
        h, lo, hi = classes[c]
        for p in range(lo, hi):
            at = (h * fold + p) * SUB
            src = sent.at[pl.ds(at, SUB), lanes(k)]
            dst = held.at[h, pl.ds(p * SUB, SUB), lanes(k)]
            remote(f"z{c}", k, src, dst, at_z[peers[h * fold + p]])

    def spread(c, k):
        if c:
            wait(f"z{c}", k, rows_of(c, 0, k))
        remote(f"x{c}", k, rows_of(c, 0, k), rows_of(c, 1, k), at_x)
        remote(f"y{c}", k, rows_of(c, 0, k), rows_of(c, 2, k), at_y)

    def forward(c, k):
        lo, mid, hi = halves(c)
        if mid > lo:
            wait(f"x{c}", k, rows_of(c, 1, k))
            remote(f"fy{c}", k, rows_of(c, 1, k, lo, mid), rows_of(c, 3, k, lo, mid), at_y)
        if hi > mid:
            wait(f"y{c}", k, rows_of(c, 2, k))
            remote(f"fx{c}", k, rows_of(c, 2, k, mid, hi), rows_of(c, 3, k, mid, hi), at_x)

    def arrived(c, k):
        lo, mid, hi = halves(c)
        if mid == hi:
            wait(f"y{c}", k, rows_of(c, 2, k))
        if lo == mid:
            wait(f"x{c}", k, rows_of(c, 1, k))
        if mid > lo:
            wait(f"fy{c}", k, rows_of(c, 3, k, lo, mid))
        if hi > mid:
            wait(f"fx{c}", k, rows_of(c, 3, k, mid, hi))

    def make(k):
        tok_cp[k].wait()
        picked = jnp.zeros((subs, WIDE), F32)
        for q in range(PARTS):
            picked += dot(place[q], tok[:, k * CHUNK + q * WIDE : k * CHUNK + (q + 1) * WIDE])
        for b in range(WIDE // QBLOCK):
            block = picked[:, b * QBLOCK : (b + 1) * QBLOCK]
            largest = jnp.max(jnp.abs(block), axis=1, keepdims=True)
            scale = ((largest + 1e-06) * (1.0 / 448.0)).astype(BF16).astype(F32)
            coded = (block / scale).astype(BF16).astype(F32)
            value = (coded * scale).astype(BF16)
            at = k * WIDE + b * QBLOCK
            sent[:, at : at + QBLOCK] = value
            held[0, 0:SUB, at : at + QBLOCK] = value[0:SUB]
        exchange(3, k)
        exchange(1, k)
        spread(0, k)
        if k == 0:
            for p in range(1, groups):
                at = pl.ds(p * SUB, SUB)
                remote("wz", 0, wsent.at[at], warr.at[at], at_z[peers[p]])

    def wspread(_):
        wait("wz", 0, warr.at[pl.ds(SUB, subs - SUB)])
        total = jnp.zeros((SUB, 128), F32)
        for p in range(groups):
            total += warr[p * SUB : (p + 1) * SUB].astype(F32)
        whold[0:SUB] = total.astype(BF16)
        remote("wx", 0, whold.at[pl.ds(0, SUB)], whold.at[pl.ds(SUB, SUB)], at_x)
        remote("wy", 0, whold.at[pl.ds(0, SUB)], whold.at[pl.ds(2 * SUB, SUB)], at_y)

    def wforward(_):
        wait("wx", 0, whold.at[pl.ds(SUB, SUB)])
        remote("wf", 0, whold.at[pl.ds(SUB, SUB)], whold.at[pl.ds(3 * SUB, SUB)], at_y)

    def warrived(_):
        wait("wy", 0, whold.at[pl.ds(2 * SUB, SUB)])
        wait("wf", 0, whold.at[pl.ds(3 * SUB, SUB)])
        er = lax.broadcasted_iota(jnp.int32, (lots, 4 * SUB), 0)
        ec = lax.broadcasted_iota(jnp.int32, (lots, 4 * SUB), 1)
        pick = ec == (er // slots) * SUB + (er % CAP) * PARTS
        spun = dot(pick.astype(F32).astype(BF16), whold[...])
        wl = lax.broadcasted_iota(jnp.int32, (lots, 128), 1)
        place_in = (lax.broadcasted_iota(jnp.int32, (lots, 128), 0) % slots) // CAP
        for h in range(2):
            far = distance(place_in + h * fold)
            for e in range(experts):
                mine = jnp.where(wl == far * experts + e, spun, 0.0)
                column = jnp.sum(mine, axis=1, keepdims=True)
                wcol[h, e] = jnp.broadcast_to(column, (lots, 128))

    def multiply(h, k):
        for c in range(4):
            if classes[c][0] == h:
                arrived(c, k)
        for u in range(4 * sh // 128):
            moved = dot(perm[...], held[h, u * 128 : (u + 1) * 128, k * WIDE : (k + 1) * WIDE])
            moved = moved.astype(BF16)
            for q in range(PARTS):
                xs[h, u * ur : (u + 1) * ur, q * WIDE : (q + 1) * WIDE] = moved[q * ur : (q + 1) * ur]
        wg_cp[k].wait() if h else None
        wu_cp[k].wait() if h else None
        cols = pl.ds(k * CHUNK, CHUNK)
        for e in range(experts):
            for s, w in enumerate((wg, wu)):
                got = dot(xs[h], w[e, cols, :])
                if k == 0:
                    acc[h, e, s] = got
                else:
                    acc[h, e, s] += got
        if k == chunks - 1:
            for e in range(experts):
                gate = acc[h, e, 0]
                hidden[h, e] = (gate / (1.0 + jnp.exp(-gate)) * acc[h, e, 1]).astype(BF16)

    def down(h, k):
        wd_cp[k].wait() if h else None
        cols = pl.ds(k * CHUNK, CHUNK)
        total = jnp.zeros((lots, CHUNK), F32)
        for e in range(experts):
            got = dot(hidden[h, e], wd[e, :, k * CHUNK : (k + 1) * CHUNK])
            total += jnp.tile(wcol[h, e], (1, CHUNK // 128)) * got
        part[h, :, cols] = total.astype(BF16)
        at = pl.ds(3 * slots, slots)
        low, high = pl.ds(k * CHUNK, side), pl.ds(k * CHUNK + side, side)
        remote(f"ra{h}", k, part.at[h, at, low], relay_a.at[h, :, pl.ds(k * side, side)], at_y)
        remote(f"rb{h}", k, part.at[h, at, high], relay_b.at[h, :, pl.ds(k * side, side)], at_x)

    def merge(h, k):
        cols = pl.ds(k * CHUNK, CHUNK)
        for kind, relay, r, got, lo, peer in (
            ("a", relay_a, 1, got_x, k * CHUNK, at_x), ("b", relay_b, 2, got_y, k * CHUNK + side, at_y),
        ):
            here = pl.ds(k * side, side)
            wait(f"r{kind}{h}", k, relay.at[h, :, here])
            at, where = pl.ds(r * slots, slots), pl.ds(lo, side)
            total = part[h, at, where].astype(F32) + relay[h, :, here].astype(F32)
            part[h, at, where] = total.astype(BF16)
            sort = "gx" if kind == "a" else "gy"
            remote(f"{sort}{h}", k, part.at[h, at, cols], got.at[h, :, cols], peer)

    def home(h, k):
        cols = pl.ds(k * CHUNK, CHUNK)
        wait(f"gx{h}", k, got_x.at[h, :, cols])
        wait(f"gy{h}", k, got_y.at[h, :, cols])
        total = (
            part[h, 0:slots, cols].astype(F32) + got_x[h, :, cols].astype(F32) + got_y[h, :, cols].astype(F32)
        ).astype(BF16)
        for u in range(sh // unit):
            stacked = jnp.concatenate(
                [total[u * tu : (u + 1) * tu, q * WIDE : (q + 1) * WIDE] for q in range(PARTS)], axis=0
            )
            moved = dot(perm_t[...], stacked).astype(BF16)
            at = h * sh + u * unit
            back_s[at : at + unit, k * WIDE : (k + 1) * WIDE] = moved
            if h == 0 and u == 0:
                back[0:SUB, k * WIDE : (k + 1) * WIDE] = moved[0:SUB]
        for p in range(h * fold, (h + 1) * fold):
            if p:
                at = pl.ds(p * SUB, SUB)
                remote(f"zr{h}", k, back_s.at[at, lanes(k)], back.at[at, lanes(k)], at_z[peers[p]])

    out_cp = [
        pltpu.make_async_copy(obuf.at[k], out_hbm.at[:, pl.ds(k * CHUNK, CHUNK)], lsems.at[4, k])
        for k in range(chunks)
    ]

    def finish(k):
        if k == 0:
            for q in range(PARTS):
                place_t[q] = place[q].astype(F32).T.astype(BF16)
        wait("zr1", k, back.at[pl.ds(sh, sh), lanes(k)])
        wait("zr0", k, back.at[pl.ds(SUB, sh - SUB), lanes(k)])
        for q in range(PARTS):
            obuf[k, :, q * WIDE : (q + 1) * WIDE] = dot(
                place_t[q], back[:, k * WIDE : (k + 1) * WIDE]
            ).astype(BF16)
        out_cp[k].start()

    stages = {"make": make, "late": lambda k: exchange(2, k), "finish": finish}
    for c in range(4):
        stages[f"spread{c}"] = functools.partial(spread, c)
        stages[f"forward{c}"] = functools.partial(forward, c)
    for h in range(2):
        for name, stage in (("multiply", multiply), ("down", down), ("merge", merge), ("home", home)):
            stages[f"{name}{h}"] = functools.partial(stage, h)
    once = {"wspread": wspread, "wforward": wforward, "warrived": warrived}
    tasks = []
    for name, (start, step) in TIMES.items():
        for k in range(1 if name in once else chunks):
            tasks.append((start + step * k, name, k))
    for _, name, k in sorted(tasks):
        (once.get(name) or stages[name])(k)

    for c in range(4):
        h, first, last = classes[c]
        lo, mid, hi = halves(c)
        if c:
            sent_all(f"z{c}", sent.at[pl.ds((h * fold + first) * SUB, (last - first) * SUB), :])
        sent_all(f"x{c}", rows_of(c, 0, None))
        sent_all(f"y{c}", rows_of(c, 0, None))
        if mid > lo:
            sent_all(f"fy{c}", rows_of(c, 1, None, lo, mid))
        if hi > mid:
            sent_all(f"fx{c}", rows_of(c, 2, None, mid, hi))
    sent_all("wz", wsent.at[pl.ds(SUB, subs - SUB)])
    for kind in ("wx", "wy", "wf"):
        sent_all(kind, whold.at[pl.ds(0, SUB)])
    for h in range(2):
        sent_all(f"ra{h}", relay_a.at[h])
        sent_all(f"rb{h}", relay_b.at[h])
        sent_all(f"gx{h}", got_x.at[h])
        sent_all(f"gy{h}", got_y.at[h])
        at = pl.ds(h * sh + (0 if h else SUB), sh - (0 if h else SUB))
        sent_all(f"zr{h}", back_s.at[at, :])
    for c in out_cp:
        c.wait()


def shards(tokens, expert_ids, route_weight, w_gate, w_up, w_down):
    groups = lax.axis_size("torus")
    rows, width = tokens.shape
    experts, _, units = w_gate.shape
    chunks = width // CHUNK
    subs = groups * SUB
    fold = groups // 2
    sh = fold * SUB
    slots = fold * CAP
    lots = 4 * slots
    span = chunks * WIDE
    anywhere = pl.BlockSpec(memory_space=pl.ANY)
    V = pltpu.VMEM
    return pl.pallas_call(
        functools.partial(kernel, groups, chunks),
        out_shape=jax.ShapeDtypeStruct((rows, width), BF16),
        in_specs=[anywhere] * 6,
        out_specs=anywhere,
        scratch_shapes=[
            V((rows, width), BF16),
            V((expert_ids.shape[1], rows), jnp.int32),
            V((expert_ids.shape[1], rows), BF16),
            V(w_gate.shape, BF16),
            V(w_up.shape, BF16),
            V(w_down.shape, BF16),
            V((PARTS, subs, rows), BF16),
            V((PARTS, rows, subs), BF16),
            V((128, 128), BF16),
            V((min(128, sh), min(128, sh)), BF16),
            V((subs, span), BF16),
            V((2, 4 * sh, span), BF16),
            V((subs, 128), BF16),
            V((subs, 128), BF16),
            V((4 * SUB, 128), BF16),
            V((2, lots, CHUNK), BF16),
            V((2, experts, 2, lots, units), F32),
            V((2, experts, lots, units), BF16),
            V((2, experts, lots, 128), F32),
            V((2, lots, width), BF16),
            V((2, slots, width // 2), BF16),
            V((2, slots, width // 2), BF16),
            V((2, slots, width), BF16),
            V((2, slots, width), BF16),
            V((subs, span), BF16),
            V((subs, span), BF16),
            V((chunks, rows, CHUNK), BF16),
            pltpu.SemaphoreType.DMA((len(KINDS),)),
            pltpu.SemaphoreType.DMA((len(KINDS), chunks)),
            pltpu.SemaphoreType.DMA((6, chunks)),
        ],
        compiler_params=pltpu.CompilerParams(
            collective_id=0, has_side_effects=True, vmem_limit_bytes=64000000
        ),
    )(tokens, expert_ids.T, route_weight.T, w_gate, w_up, w_down)


def solution(mesh):
    placed = (
        P(("node", "torus"), None),
        P(("node", "torus"), None),
        P(("node", "torus"), None),
        P("torus", None, "node"),
        P("torus", None, "node"),
        P("torus", "node", None),
    )
    return jax.shard_map(
        shards, mesh=mesh, in_specs=placed, out_specs=P(("node", "torus"), None), check_vma=False
    )
```

```python
import functools

import jax
import jax.numpy as jnp
from jax import lax
from jax.experimental import pallas as pl
from jax.experimental.pallas import tpu as pltpu
from jax.sharding import PartitionSpec as P

CAP = 4
QBLOCK = 128
PARTS = 4
SUB = CAP * PARTS
CHUNK = 1024
WIDE = CHUNK // PARTS
MESH = pl.DeviceIdType.MESH
F32 = jnp.float32
BF16 = jnp.bfloat16

KINDS = ("z1", "z2", "z3", "t0", "t1", "t2", "t3", "a0", "a1", "r0", "r1", "g0", "g1", "zr")
EARLY = 4

PLACES = {
    "make": (0, 1, 2, 4, 5, 6, 9),
    "spread1": (3, 7, 8, 11, 12, 15, 57),
    "forward0": (10, 13, 49, 52, 54, 55, 65),
    "late": (14, 17, 19, 21, 23, 35, 38),
    "spread3": (16, 22, 24, 25, 26, 28, 30),
    "wspread": (18,),
    "forward1": (20, 46, 50, 51, 56, 61, 77),
    "wforward": (27,),
    "forward3": (29, 31, 32, 34, 36, 39, 43),
    "spread2": (33, 40, 42, 44, 45, 59, 63),
    "warrived": (37,),
    "multiply1": (41, 47, 48, 53, 60, 62, 67),
    "forward2": (58, 64, 66, 68, 69, 75, 78),
    "down1": (70, 71, 72, 73, 74, 76, 79),
    "multiply0": (80, 82, 84, 86, 87, 90, 91),
    "merge1": (81, 83, 85, 88, 89, 97, 112),
    "down0": (92, 93, 94, 95, 96, 100, 104),
    "home1": (98, 99, 103, 105, 107, 109, 120),
    "merge0": (101, 102, 106, 108, 110, 111, 115),
    "home0": (113, 114, 116, 117, 118, 119, 122),
    "finish": (121, 123, 124, 125, 126, 127, 128),
}


def flipped(index, mask):
    value = index
    bit = 0
    while mask >> bit:
        if (mask >> bit) & 1:
            size = 1 << bit
            value = value + size * (1 - 2 * lax.rem(lax.div(index, jnp.int32(size)), jnp.int32(2)))
        bit += 1
    return value


def dot(left, right):
    return jnp.dot(left, right, preferred_element_type=F32)


def kernel(
    groups, chunks,
    tok_hbm, ids_hbm, rw_hbm, wg_hbm, wu_hbm, wd_hbm, out,
    tok, ids, rw, wgu, wd, place, place_t, perm, perm_t,
    sent, held, wsent, warr, whold, xs, acc, hidden, wcol,
    part, relay, got, back_s, back,
    ssems, rsems, wsems, lsems,
):
    node = lax.axis_index("node")
    torus = lax.axis_index("torus")
    rows = tok.shape[0]
    subs = groups * SUB
    fold = groups // 2
    sh = fold * SUB
    slots = fold * CAP
    lots = 4 * slots
    side = CHUNK // 2
    unit = min(128, sh)
    experts = wd.shape[0]
    peers = [j for j in range(groups) if not j & 2] + [j for j in range(groups) if j & 2]
    at_x = (flipped(node, 1), torus)
    at_y = (flipped(node, 2), torus)
    at_z = [(node, flipped(torus, j)) for j in range(groups)]

    barrier = pltpu.get_barrier_semaphore()
    for peer in at_z[1:] + [at_x, at_y]:
        pl.semaphore_signal(barrier, inc=1, device_id=peer, device_id_type=MESH)

    def load(src, dst, at):
        pltpu.make_async_copy(src, dst, lsems.at[at]).start()

    def loaded(ref, at):
        pltpu.make_async_copy(ref, ref, lsems.at[at]).wait()

    load(ids_hbm, ids, 0)
    load(rw_hbm, rw, 1)
    spans = [pl.ds(k * CHUNK, CHUNK) for k in range(chunks)]
    for cols in spans:
        load(tok_hbm.at[:, cols], tok.at[:, cols], 2)
    for cols in spans:
        load(wg_hbm.at[:, cols, :], wgu.at[0, :, cols, :], 3)
        load(wu_hbm.at[:, cols, :], wgu.at[1, :, cols, :], 3)
    for cols in spans:
        load(wd_hbm.at[:, :, cols], wd.at[:, :, cols], 4)

    pr = lax.broadcasted_iota(jnp.int32, (128, 128), 0)
    pc = lax.broadcasted_iota(jnp.int32, (128, 128), 1)
    ur = 128 // PARTS
    perm[...] = (pc == (pr % ur) * PARTS + pr // ur).astype(F32).astype(BF16)
    tr = lax.broadcasted_iota(jnp.int32, (unit, unit), 0)
    tc = lax.broadcasted_iota(jnp.int32, (unit, unit), 1)
    tu = unit // PARTS
    perm_t[...] = (tr == (tc % tu) * PARTS + tc // tu).astype(F32).astype(BF16)

    def distance(at):
        inner = at % fold
        return (inner // 2) * 4 + (at // fold) * 2 + inner % 2

    loaded(ids, 0)
    loaded(rw, 1)
    row = lax.broadcasted_iota(jnp.int32, (subs, rows), 0)
    gid = jnp.bitwise_xor(distance(row // SUB), jnp.full((subs, rows), torus, jnp.int32))
    slot_of = (row // PARTS) % CAP
    part_of = row % PARTS
    hit = jnp.zeros((subs, rows), F32)
    chosen = [jnp.zeros((subs, rows), F32) for _ in range(experts)]
    weights = rw[...].astype(F32)
    for k in range(ids.shape[0]):
        named = jnp.broadcast_to(ids[k : k + 1, :], (subs, rows))
        weight = jnp.broadcast_to(weights[k : k + 1, :], (subs, rows))
        for e in range(experts):
            same = named == gid * experts + e
            hit = jnp.where(same, 1.0, hit)
            chosen[e] = jnp.where(same, weight, chosen[e])
    lower = lax.broadcasted_iota(jnp.int32, (rows, rows), 0) < lax.broadcasted_iota(
        jnp.int32, (rows, rows), 1
    )
    before = dot(hit.astype(BF16), lower.astype(F32).astype(BF16))
    onehot = jnp.where(before == slot_of.astype(F32), hit, 0.0)
    for q in range(PARTS):
        place[q] = jnp.where(part_of == q, onehot, 0.0).astype(BF16)
    lane = lax.broadcasted_iota(jnp.int32, (subs, 128), 1)
    from_j = distance(lax.broadcasted_iota(jnp.int32, (subs, 128), 0) // SUB)
    wrow = jnp.zeros((subs, 128), F32)
    for e in range(experts):
        total = jnp.sum(onehot * chosen[e], axis=1, keepdims=True)
        wrow = jnp.where(lane == from_j * experts + e, total, wrow)
    wsent[...] = wrow.astype(BF16)
    warr[0:SUB] = wrow[0:SUB].astype(BF16)

    def build(k):
        picked = jnp.zeros((subs, WIDE), F32)
        for q in range(PARTS):
            picked += dot(place[q], tok[:, k * CHUNK + q * WIDE : k * CHUNK + (q + 1) * WIDE])
        for b in range(WIDE // QBLOCK):
            block = picked[:, b * QBLOCK : (b + 1) * QBLOCK]
            largest = jnp.max(jnp.abs(block), axis=1, keepdims=True)
            scale = ((largest + 1e-06) * (1.0 / 448.0)).astype(BF16).astype(F32)
            coded = (block / scale).astype(BF16).astype(F32)
            value = (coded * scale).astype(BF16)
            at = k * WIDE + b * QBLOCK
            sent[:, at : at + QBLOCK] = value
            held[0:SUB, at : at + QBLOCK] = value[0:SUB]

    loaded(tok, 2)
    for k in range(EARLY):
        build(k)

    pl.semaphore_wait(barrier, groups + 1)

    def copy(src, dst, send, recv, peer):
        pltpu.make_async_remote_copy(
            src_ref=src, dst_ref=dst, send_sem=send, recv_sem=recv,
            device_id=peer, device_id_type=MESH,
        ).start()

    def remote(kind, k, src, dst, peer):
        late = 1 if kind[0] in "rg" or kind == "zr" else 0
        copy(src, dst, ssems.at[late], rsems.at[KINDS.index(kind), k], peer)

    def wait(kind, k, ref):
        pltpu.make_async_copy(ref, ref, rsems.at[KINDS.index(kind), k]).wait()

    def settle(ref, sem):
        pltpu.make_async_copy(ref, ref, sem).wait()

    def lanes(k):
        return pl.ds(k * WIDE, WIDE)

    classes = ((0, 0, 1), (0, 1, 2), (0, 2, fold), (1, 0, fold))

    def some(count, k):
        return held.at[pl.ds(0, count), lanes(k)]

    def rows_of(c, r, k, lo=None, hi=None):
        h, first, last = classes[c]
        lo = first if lo is None else lo
        hi = last if hi is None else hi
        return held.at[pl.ds((h * 4 + r) * sh + lo * SUB, (hi - lo) * SUB), lanes(k)]

    def exchange(c, k):
        h, lo, hi = classes[c]
        for p in range(lo, hi):
            src = sent.at[pl.ds((h * fold + p) * SUB, SUB), lanes(k)]
            dst = held.at[pl.ds(h * 4 * sh + p * SUB, SUB), lanes(k)]
            remote(f"z{c}", k, src, dst, at_z[peers[h * fold + p]])

    def spread(c, k):
        if c:
            wait(f"z{c}", k, rows_of(c, 0, k))
        by_x = "a0" if c == 1 else f"t{c}"
        by_y = "a0" if c == 0 else f"t{c}"
        remote(by_x, k, rows_of(c, 0, k), rows_of(c, 1, k), at_x)
        remote(by_y, k, rows_of(c, 0, k), rows_of(c, 2, k), at_y)

    def forward(c, k):
        h, lo, hi = classes[c]
        wait(f"t{c}", k, some((hi - lo) * SUB * (1 if c < 2 else 2), k))
        mid = {0: hi, 1: lo}.get(c, (lo + hi) // 2)
        if mid > lo:
            remote(f"a{h}", k, rows_of(c, 1, k, lo, mid), rows_of(c, 3, k, lo, mid), at_y)
        if hi > mid:
            remote(f"a{h}", k, rows_of(c, 2, k, mid, hi), rows_of(c, 3, k, mid, hi), at_x)

    def make(k):
        if k >= EARLY:
            build(k)
        exchange(3, k)
        exchange(1, k)
        spread(0, k)
        if k == 0:
            for p in range(1, groups):
                at = pl.ds(p * SUB, SUB)
                copy(wsent.at[at], warr.at[at], ssems.at[2], wsems.at[0], at_z[peers[p]])

    def wspread(_):
        settle(warr.at[pl.ds(SUB, subs - SUB)], wsems.at[0])
        total = jnp.zeros((SUB, 128), F32)
        for p in range(groups):
            total += warr[p * SUB : (p + 1) * SUB].astype(F32)
        whold[0:SUB] = total.astype(BF16)
        own = whold.at[pl.ds(0, SUB)]
        copy(own, whold.at[pl.ds(SUB, SUB)], ssems.at[3], wsems.at[1], at_x)
        copy(own, whold.at[pl.ds(2 * SUB, SUB)], ssems.at[3], wsems.at[2], at_y)

    def wforward(_):
        near = whold.at[pl.ds(SUB, SUB)]
        settle(near, wsems.at[1])
        copy(near, whold.at[pl.ds(3 * SUB, SUB)], ssems.at[3], wsems.at[2], at_y)

    def warrived(_):
        settle(whold.at[pl.ds(2 * SUB, 2 * SUB)], wsems.at[2])
        er = lax.broadcasted_iota(jnp.int32, (lots, 4 * SUB), 0)
        ec = lax.broadcasted_iota(jnp.int32, (lots, 4 * SUB), 1)
        pick = ec == (er // slots) * SUB + (er % CAP) * PARTS
        spun = dot(pick.astype(F32).astype(BF16), whold[...])
        wl = lax.broadcasted_iota(jnp.int32, (lots, 128), 1)
        place_in = (lax.broadcasted_iota(jnp.int32, (lots, 128), 0) % slots) // CAP
        for h in range(2):
            far = distance(place_in + h * fold)
            for e in range(experts):
                mine = jnp.where(wl == far * experts + e, spun, 0.0)
                column = jnp.sum(mine, axis=1, keepdims=True)
                wcol[h, e] = jnp.broadcast_to(column, (lots, 128))

    def multiply(h, k):
        if h:
            wait("a1", k, some(sh, k))
        else:
            wait("a0", k, some(sh + 2 * SUB, k))
        for u in range(4 * sh // 128):
            at = h * 4 * sh + u * 128
            moved = dot(perm[...], held[at : at + 128, k * WIDE : (k + 1) * WIDE]).astype(BF16)
            for q in range(PARTS):
                xs[h, u * ur : (u + 1) * ur, q * WIDE : (q + 1) * WIDE] = moved[q * ur : (q + 1) * ur]
        if h and k == 0:
            loaded(wgu, 3)
        cols = pl.ds(k * CHUNK, CHUNK)
        for e in range(experts):
            for s in range(2):
                term = dot(xs[h], wgu[s, e, cols, :])
                if k == 0:
                    acc[h, e, s] = term
                else:
                    acc[h, e, s] += term
        if k == chunks - 1:
            for e in range(experts):
                gate = acc[h, e, 0]
                hidden[h, e] = (gate / (1.0 + jnp.exp(-gate)) * acc[h, e, 1]).astype(BF16)

    def down(h, k):
        if h and k == 0:
            loaded(wd, 4)
        total = jnp.zeros((lots, CHUNK), F32)
        for e in range(experts):
            term = dot(hidden[h, e], wd[e, :, k * CHUNK : (k + 1) * CHUNK])
            total += jnp.tile(wcol[h, e], (1, CHUNK // 128)) * term
        part[h, :, spans[k]] = total.astype(BF16)
        here = pl.ds(k * side, side)
        for s, peer in enumerate((at_y, at_x)):
            src = part.at[h, pl.ds(3 * slots, slots), pl.ds(k * CHUNK + s * side, side)]
            remote(f"r{h}", k, src, relay.at[h, s, :, here], peer)

    def merge(h, k):
        here = pl.ds(k * side, side)
        wait(f"r{h}", k, relay.at[h, :, :, here])
        for s, peer in enumerate((at_x, at_y)):
            at, where = pl.ds((s + 1) * slots, slots), pl.ds(k * CHUNK + s * side, side)
            total = part[h, at, where].astype(F32) + relay[h, s, :, here].astype(F32)
            part[h, at, where] = total.astype(BF16)
            remote(f"g{h}", k, part.at[h, at, spans[k]], got.at[h, s, :, spans[k]], peer)

    def home(h, k):
        cols = spans[k]
        wait(f"g{h}", k, got.at[h, :, :, cols])
        total = (
            part[h, 0:slots, cols].astype(F32) + got[h, 0, :, cols].astype(F32) + got[h, 1, :, cols].astype(F32)
        ).astype(BF16)
        for u in range(sh // unit):
            stacked = jnp.concatenate(
                [total[u * tu : (u + 1) * tu, q * WIDE : (q + 1) * WIDE] for q in range(PARTS)], axis=0
            )
            moved = dot(perm_t[...], stacked).astype(BF16)
            at = h * sh + u * unit
            back_s[at : at + unit, k * WIDE : (k + 1) * WIDE] = moved
            if h == 0 and u == 0:
                back[0:SUB, k * WIDE : (k + 1) * WIDE] = moved[0:SUB]
        for p in range(h * fold, (h + 1) * fold):
            if p:
                at = pl.ds(p * SUB, SUB)
                remote("zr", k, back_s.at[at, lanes(k)], back.at[at, lanes(k)], at_z[peers[p]])

    def finish(k):
        if k == 0:
            for q in range(PARTS):
                place_t[q] = place[q].astype(F32).T.astype(BF16)
        wait("zr", k, back.at[pl.ds(SUB, subs - SUB), lanes(k)])
        for q in range(PARTS):
            at = k * CHUNK + q * WIDE
            out[:, at : at + WIDE] = dot(place_t[q], back[:, k * WIDE : (k + 1) * WIDE]).astype(BF16)

    stages = {"make": make, "late": lambda k: exchange(2, k), "finish": finish}
    for c in range(4):
        stages[f"spread{c}"] = functools.partial(spread, c)
        stages[f"forward{c}"] = functools.partial(forward, c)
    for h in range(2):
        for name, stage in (("multiply", multiply), ("down", down), ("merge", merge), ("home", home)):
            stages[f"{name}{h}"] = functools.partial(stage, h)
    once = {"wspread": wspread, "wforward": wforward, "warrived": warrived}
    tasks = [(at, name, k) for name, places in PLACES.items() for k, at in enumerate(places)]
    for _, name, k in sorted(tasks):
        (once.get(name) or stages[name])(k)

    for late in range(2):
        settle(held.at[pl.ds(SUB, 8 * sh - SUB)], ssems.at[late])
    settle(wsent.at[pl.ds(SUB, subs - SUB)], ssems.at[2])
    settle(whold.at[pl.ds(SUB, 3 * SUB)], ssems.at[3])


def shards(tokens, expert_ids, route_weight, w_gate, w_up, w_down):
    groups = lax.axis_size("torus")
    rows, width = tokens.shape
    experts, _, units = w_gate.shape
    chunks = width // CHUNK
    subs = groups * SUB
    fold = groups // 2
    sh = fold * SUB
    slots = fold * CAP
    lots = 4 * slots
    span = chunks * WIDE
    anywhere = pl.BlockSpec(memory_space=pl.ANY)
    args = (tokens, expert_ids.T, route_weight.T, w_gate, w_up, w_down)
    V = pltpu.VMEM
    return pl.pallas_call(
        functools.partial(kernel, groups, chunks),
        out_shape=pltpu.VMEM((rows, width), BF16),
        in_specs=[anywhere] * 6,
        out_specs=pl.BlockSpec(memory_space=pltpu.VMEM),
        scratch_shapes=[
            V((rows, width), BF16),
            V((expert_ids.shape[1], rows), jnp.int32),
            V((expert_ids.shape[1], rows), BF16),
            V((2,) + w_gate.shape, BF16),
            V(w_down.shape, BF16),
            V((PARTS, subs, rows), BF16),
            V((PARTS, rows, subs), BF16),
            V((128, 128), BF16),
            V((min(128, sh), min(128, sh)), BF16),
            V((subs, span), BF16),
            V((8 * sh, span), BF16),
            V((subs, 128), BF16),
            V((subs, 128), BF16),
            V((4 * SUB, 128), BF16),
            V((2, lots, CHUNK), BF16),
            V((2, experts, 2, lots, units), F32),
            V((2, experts, lots, units), BF16),
            V((2, experts, lots, 128), F32),
            V((2, lots, width), BF16),
            V((2, 2, slots, width // 2), BF16),
            V((2, 2, slots, width), BF16),
            V((subs, span), BF16),
            V((subs, span), BF16),
            pltpu.SemaphoreType.DMA((4,)),
            pltpu.SemaphoreType.DMA((len(KINDS), chunks)),
            pltpu.SemaphoreType.DMA((3,)),
            pltpu.SemaphoreType.DMA((5,)),
        ],
        compiler_params=pltpu.CompilerParams(
            collective_id=0, has_side_effects=True, vmem_limit_bytes=60000000
        ),
    )(*[pltpu.with_memory_space_constraint(a, pltpu.HBM) for a in args])


def solution(mesh):
    placed = (
        P(("node", "torus"), None),
        P(("node", "torus"), None),
        P(("node", "torus"), None),
        P("torus", None, "node"),
        P("torus", None, "node"),
        P("torus", "node", None),
    )
    return jax.shard_map(
        shards, mesh=mesh, in_specs=placed, out_specs=P(("node", "torus"), None), check_vma=False
    )
```
